32 devices in a mesh: dp: 16 (over z, x, core), tensor: 2 (over y).
Axes of the slice: x: 2, y: 2, z: 4, core: 2. Of those that a mesh axis runs over, the one named last changes fastest.
Arguments:
- grad_hidden: bfloat16 [2048, 14336], P('dp', 'tensor'), may hold values from -18 to 18
- gate: bfloat16 [2048, 14336], P('dp', 'tensor'), may hold values from -6 to 6
Outputs:
- factor: float32 [14336, 14336], P('tensor', 'dp')
The draws below stay inside these ranges and needn't reach their ends.
All inputs are finite; a program needn't handle non-finite values.
Results may differ from the reference program's by a relative error of at most 0.0065.
Values may be sent and summed in bfloat16 or wider, within the bound.
A program may use at most 128 MiB of HBM per device.

```python
import jax
import jax.numpy as jnp
from jax import lax

FF = 14336
TOKENS = 2048


def level_of(rng, extent, split, least, high):
    gain, own = 1.0, jax.random.fold_in(rng, 6)
    for dim, blocks in split:
        draws = jnp.exp(jax.random.uniform(jax.random.fold_in(own, dim), (blocks,), jnp.float32, least / len(split), high / len(split)))
        gain = gain * jnp.repeat(draws, extent[dim] // blocks).reshape([-1 if axis == dim else 1 for axis in range(len(extent))])
    return gain


def bell_draw(stream_key, dims, scale, most, shards=(), dtype=jnp.bfloat16):
    array = jax.random.normal(stream_key, dims, jnp.float32) * scale
    if len(shards) > 0:
        array = level_of(stream_key, dims, shards, -0.22, 0.18) * array
    return jnp.clip(array, min=-most, max=most).astype(dtype)


def setup_inputs(seed: int = 0) -> dict:
    splits = jax.random.split(jax.random.key(seed), 3)
    return {
        "grad_hidden": bell_draw(splits[0], (TOKENS, FF), 3.0, 18.0, ((0, 16), (1, 2))),
        "gate": bell_draw(splits[1], (TOKENS, FF), 1.0, 6.0, ((0, 16), (1, 2))),
    }


def reference(grad_hidden, gate):
    up_grad = (grad_hidden.astype(jnp.float32) * jax.nn.silu(gate.astype(jnp.float32))).astype(jnp.bfloat16)
    wide = up_grad.astype(jnp.float32)
    blocks = wide.reshape(wide.shape[0], FF // 1792 if FF % 1792 == 0 else 1, -1)
    blocks = jnp.transpose(blocks, (1, 0, 2))

    def column_block(piece):
        return jnp.dot(wide.T, piece, precision=lax.Precision.HIGHEST, preferred_element_type=jnp.float32)

    panels = lax.map(column_block, blocks)
    factor = jnp.transpose(panels, (1, 0, 2)).reshape(FF, FF)
    return factor / TOKENS
```

```python
import functools

import jax
import jax.numpy as jnp
from jax import lax
from jax.experimental import pallas as pl
from jax.experimental.pallas import tpu as pltpu
from jax.sharding import PartitionSpec as P

MESH = pl.DeviceIdType.MESH
LANES = 128


def activations(grad_hidden, gate):
    return (grad_hidden.astype(jnp.float32) * jax.nn.silu(gate.astype(jnp.float32))).astype(
        jnp.bfloat16
    )


def plain(grad_hidden, gate):
    up_grad = activations(grad_hidden, gate)
    tensor_count = lax.axis_size("tensor")
    data_count = lax.axis_size("dp")
    col_width = up_grad.shape[1] * tensor_count // data_count
    ratio = data_count // tensor_count
    data_index = lax.axis_index("dp")
    owner = data_index // ratio
    offset = data_index % ratio * col_width
    contract = (((0,), (0,)), ((), ()))
    total_tokens = up_grad.shape[0] * data_count
    rows_all = lax.all_gather(up_grad, "dp", axis=0, tiled=True)
    panel = lax.dynamic_slice_in_dim(rows_all, offset, col_width, 1)
    slices = lax.all_gather(panel, "tensor", axis=1, tiled=True)
    cols_all = lax.dynamic_slice_in_dim(slices, owner * col_width, col_width, 1)
    summed = lax.dot_general(rows_all, cols_all, contract, preferred_element_type=jnp.float32)
    return summed / total_tokens


def flip_kernel(g_ref, v_ref, o_ref):
    v = v_ref[...].astype(jnp.float32)
    u = g_ref[...].astype(jnp.float32) * (v / (1.0 + jnp.exp(-v)))
    o_ref[...] = u.astype(jnp.bfloat16).T


def flip(grad_hidden, gate, width):
    tokens, hidden = grad_hidden.shape
    return pl.pallas_call(
        flip_kernel,
        grid=(hidden // width,),
        in_specs=[pl.BlockSpec((tokens, width), lambda i: (0, i))] * 2,
        out_specs=pl.BlockSpec((width, tokens), lambda i: (i, 0)),
        out_shape=jax.ShapeDtypeStruct((hidden, tokens), jnp.bfloat16),
    )(grad_hidden, gate)


def gather_kernel(dims, own_ref, all_ref, panel_ref, own_sem, z_send, x_send, c_send, y_send, recv, c_recv, y_recv):
    line, count, cross, rows = dims
    first = count - cross
    me, t = lax.axis_index("dp"), lax.axis_index("tensor")
    z, x, core = me // 4, me // 2 % 2, me % 2
    chips = 2 * line
    at = lambda zz, xx: zz * 2 + xx
    here = at(z, x)
    owns = (here // (chips // 2)) == t
    part = here % (chips // 2)
    per = count // (chips // 2)

    up = (jnp.minimum(z + 1, line - 1) * 4 + x * 2 + core, t)
    down = (jnp.maximum(z - 1, 0) * 4 + x * 2 + core, t)
    over = (z * 4 + (1 - x) * 2 + core, t)
    twin = (z * 4 + x * 2 + 1 - core, t)
    has_up, has_down = z < line - 1, z > 0

    barrier = pltpu.get_barrier_semaphore()
    greet = lambda dev: pl.semaphore_signal(barrier, inc=1, device_id=dev, device_id_type=MESH)
    greet(over)
    greet(twin)
    greet((me, 1 - t))
    greet(twin[:1] + (1 - t,))
    pl.when(has_up)(lambda: greet(up))
    pl.when(has_down)(lambda: greet(down))
    end = (z == 0) | (z == line - 1)
    pl.semaphore_wait(barrier, jnp.where(end, 5, 6))

    def rows_of(k):
        return pl.ds(pl.multiple_of(k * rows, rows), rows)

    def lanes_of(q):
        return pl.ds(pl.multiple_of((q * 2 + core) * LANES, LANES), LANES)

    def place(q, k):
        return all_ref.at[rows_of(k), lanes_of(q)]

    def source(q, k, own):
        return own_ref.at[rows_of(k)] if own else place(q, k)

    def along(q, k, way, own=False):
        return pltpu.make_async_remote_copy(
            src_ref=source(q, k, own), dst_ref=place(q, k), send_sem=z_send.at[way, q, k],
            recv_sem=recv.at[q, k], device_id=(down, up)[way], device_id_type=MESH)

    def across(q, k, own=False):
        return pltpu.make_async_remote_copy(
            src_ref=source(q, k, own), dst_ref=place(q, k), send_sem=x_send.at[q, k],
            recv_sem=recv.at[q, k], device_id=over, device_id_type=MESH)

    def to_twin(q, k, own=False):
        return pltpu.make_async_remote_copy(
            src_ref=source(q, k, own), dst_ref=place(q, k), send_sem=c_send.at[q, k],
            recv_sem=c_recv.at[q, k], device_id=twin, device_id_type=MESH)

    def to_panel(q, k, own=False):
        j = k % per
        half = per // 2
        return pltpu.make_async_remote_copy(
            src_ref=source(q, k, own),
            dst_ref=panel_ref.at[rows_of(j % half), lanes_of(q)],
            send_sem=y_send.at[q, j], recv_sem=y_recv.at[q * 2 + core, j % half],
            device_id=(here * 2 + j // half, 1 - t), device_id_type=MESH)

    def spread(q, k, own=False):
        to_twin(q, k, own).start()
        pl.when(owns & (k // per == part))(lambda: to_panel(q, k, own).start())

    def arrive(q, k):
        across(q, k).wait_recv()

    keep = pltpu.make_async_copy(own_ref, all_ref.at[:, lanes_of(here)], own_sem)

    @pl.loop(0, count)
    def _(k):
        pl.when(has_up)(lambda: along(here, k, 1, True).start())
        pl.when(has_down)(lambda: along(here, k, 0, True).start())
        across(here, k, True).start()
        spread(here, k, True)

    keep.start()

    def from_line(s, k, way):
        zz = z - s if way else z + s
        valid = (zz >= 0) & (zz < line)

        @pl.when(valid)
        def _():
            q = at(zz, x)
            arrive(q, k)
            pl.when(has_up if way else has_down)(lambda: along(q, k, way).start())
            pl.when(k < first)(lambda: across(q, k).start())
            spread(q, k)

    def from_cross(s, k, way):
        zz = z - s if way else z + s
        valid = (zz >= 0) & (zz < line)

        @pl.when(valid)
        def _():
            q = at(zz, 1 - x)
            arrive(q, k)
            pl.when(has_up if way else has_down)(lambda: along(q, k, way).start())
            spread(q, k)

    def relayed(s, k):
        for zz in (z - s, z + s):
            @pl.when((zz >= 0) & (zz < line))
            def _():
                q = at(zz, 1 - x)
                arrive(q, k)
                spread(q, k)

    for s in range(1, line + 2):
        @pl.loop(0, count)
        def _(k):
            if s < line:
                from_line(s, k, 1)
                from_line(s, k, 0)
            if s == 1:
                q = at(z, 1 - x)
                arrive(q, k)
                spread(q, k)
            else:
                @pl.when(k < first)
                def _():
                    if s - 1 < line:
                        pl.when(end)(lambda: relayed(s - 1, k))
                    if 1 <= s - 2 < line:
                        pl.when(jnp.logical_not(end))(lambda: relayed(s - 2, k))

        if s <= line:
            @pl.loop(first, count)
            def _(k):
                if s == 1:
                    q = at(z, 1 - x)
                    pl.when(has_up)(lambda: along(q, k, 1).start())
                    pl.when(has_down)(lambda: along(q, k, 0).start())
                else:
                    from_cross(s - 1, k, 1)
                    from_cross(s - 1, k, 0)

    keep.wait()

    @pl.loop(0, chips)
    def _(q):
        zz, xx = q // 2, q % 2

        @pl.loop(0, count)
        def _(k):
            to_twin(q, k).wait()
            mine = xx == x
            pl.when((mine | (zz == z)) & ((k < first) | (zz == z)) & mine)(lambda: across(q, k).wait_send())
            goes = mine | (k >= first)
            pl.when(goes & has_up & (zz <= z))(lambda: along(q, k, 1).wait_send())
            pl.when(goes & has_down & (zz >= z))(lambda: along(q, k, 0).wait_send())
            pl.when(owns & (k // per == part))(lambda: to_panel(q, k).wait_send())

        @pl.loop(0, per // 2)
        def _(j):
            @pl.when(jnp.logical_not(owns))
            def _():
                for c in range(2):
                    piece = panel_ref.at[rows_of(j), pl.ds(pl.multiple_of((q * 2 + c) * LANES, LANES), LANES)]
                    pltpu.make_async_copy(piece, piece, y_recv.at[q * 2 + c, j]).wait()


def gather(own, dims, width, tokens):
    line, count, cross, rows = dims
    chips = 2 * line
    per = count // line
    sem = pltpu.SemaphoreType.DMA
    hidden = own.shape[0]
    return pl.pallas_call(
        functools.partial(gather_kernel, dims),
        out_shape=(
            jax.ShapeDtypeStruct((hidden, tokens), jnp.bfloat16),
            jax.ShapeDtypeStruct((width, tokens), jnp.bfloat16),
        ),
        in_specs=[pl.BlockSpec(memory_space=pl.ANY)],
        out_specs=(pl.BlockSpec(memory_space=pl.ANY),) * 2,
        scratch_shapes=[
            sem(()),
            sem((2, chips, count)),
            sem((chips, count)),
            sem((chips, count)),
            sem((chips, per)),
            sem((chips, count)),
            sem((chips, count)),
            sem((2 * chips, per // 2)),
        ],
        compiler_params=pltpu.CompilerParams(collective_id=0, has_side_effects=True),
    )(own)


def matmul_kernel(total, width, a_ref, all_ref, panel_ref, o_ref, b_ref, sem):
    me, t = lax.axis_index("dp"), lax.axis_index("tensor")
    ratio = lax.axis_size("dp") // lax.axis_size("tensor")

    @pl.when(pl.program_id(0) == 0)
    def _():
        owns = me // ratio == t

        @pl.when(owns)
        def _():
            rows = pl.ds(pl.multiple_of(me % ratio * width, LANES), width)
            pltpu.async_copy(all_ref.at[rows], b_ref, sem).wait()

        @pl.when(jnp.logical_not(owns))
        def _():
            pltpu.async_copy(panel_ref, b_ref, sem).wait()

    o_ref[...] = lax.dot_general(
        a_ref[...], b_ref[...], (((1,), (1,)), ((), ())), preferred_element_type=jnp.float32
    ) * (1.0 / total)


def matmul(everything, panel, tile):
    hidden, tokens = everything.shape
    width = panel.shape[0]
    return pl.pallas_call(
        functools.partial(matmul_kernel, tokens, width),
        grid=(hidden // tile,),
        in_specs=[
            pl.BlockSpec((tile, tokens), lambda i: (i, 0)),
            pl.BlockSpec(memory_space=pl.ANY),
            pl.BlockSpec(memory_space=pl.ANY),
        ],
        out_specs=pl.BlockSpec((tile, width), lambda i: (i, 0)),
        out_shape=jax.ShapeDtypeStruct((hidden, width), jnp.float32),
        scratch_shapes=[pltpu.VMEM((width, tokens), jnp.bfloat16), pltpu.SemaphoreType.DMA(())],
        compiler_params=pltpu.CompilerParams(vmem_limit_bytes=48 * 2**20),
    )(everything, everything, panel)


def shards(grad_hidden, gate):
    tensor_count, data_count = lax.axis_size("tensor"), lax.axis_size("dp")
    mine, hidden = grad_hidden.shape
    width = hidden * tensor_count // data_count
    tokens = mine * data_count
    count = data_count
    fits = (
        tensor_count == 2 and data_count % 4 == 0 and data_count > 4 and mine == LANES and width % LANES == 0
        and hidden % (16 * count) == 0 and tokens & (tokens - 1) == 0 and hidden % 1024 == 0
    )
    if not fits:
        return plain(grad_hidden, gate)
    line = data_count // 4
    cross = round(count / (2 * (line - 1)))
    dims = (line, count, cross, hidden // count)
    own = flip(grad_hidden, gate, 1024)
    everything, panel = gather(own, dims, width, tokens)
    return matmul(everything, panel, 1024)


def solution(mesh):
    return jax.shard_map(
        shards,
        mesh=mesh,
        in_specs=(P("dp", "tensor"), P("dp", "tensor")),
        out_specs=P("tensor", "dp"),
        check_vma=False,
    )
```

```python
import functools

import jax
import jax.numpy as jnp
from jax import lax
from jax.experimental import pallas as pl
from jax.experimental.pallas import tpu as pltpu
from jax.sharding import PartitionSpec as P

MESH = pl.DeviceIdType.MESH
LANES = 128


def activations(grad_hidden, gate):
    return (grad_hidden.astype(jnp.float32) * jax.nn.silu(gate.astype(jnp.float32))).astype(
        jnp.bfloat16
    )


def plain(grad_hidden, gate):
    up_grad = activations(grad_hidden, gate)
    tensor_count = lax.axis_size("tensor")
    data_count = lax.axis_size("dp")
    col_width = up_grad.shape[1] * tensor_count // data_count
    ratio = data_count // tensor_count
    data_index = lax.axis_index("dp")
    owner = data_index // ratio
    offset = data_index % ratio * col_width
    contract = (((0,), (0,)), ((), ()))
    total_tokens = up_grad.shape[0] * data_count
    rows_all = lax.all_gather(up_grad, "dp", axis=0, tiled=True)
    panel = lax.dynamic_slice_in_dim(rows_all, offset, col_width, 1)
    slices = lax.all_gather(panel, "tensor", axis=1, tiled=True)
    cols_all = lax.dynamic_slice_in_dim(slices, owner * col_width, col_width, 1)
    summed = lax.dot_general(rows_all, cols_all, contract, preferred_element_type=jnp.float32)
    return summed / total_tokens


def flip_kernel(g_ref, v_ref, o_ref):
    v = v_ref[...].astype(jnp.float32)
    u = g_ref[...].astype(jnp.float32) * (v / (1.0 + jnp.exp(-v)))
    o_ref[...] = u.astype(jnp.bfloat16).T


def flip(grad_hidden, gate, width):
    tokens, hidden = grad_hidden.shape
    return pl.pallas_call(
        flip_kernel,
        grid=(hidden // width,),
        in_specs=[pl.BlockSpec((tokens, width), lambda i: (0, i))] * 2,
        out_specs=pl.BlockSpec((width, tokens), lambda i: (i, 0)),
        out_shape=jax.ShapeDtypeStruct((hidden, tokens), jnp.bfloat16),
    )(grad_hidden, gate)


def early(line, z, x):
    near = jnp.where(z == 0, 1, z - 1)
    next_near = jnp.where(z == 0, 2, jnp.where(z == line - 1, line - 3, z + 1))
    return [z * 2 + x, z * 2 + 1 - x, near * 2 + x, next_near * 2 + x]


def late(line, z, x):
    low = jnp.where(z == 0, 0, jnp.where(z == line - 1, line - 3, z - 1))
    rest = [(i + jnp.where(i >= low, 3, 0)) * 2 + x for i in range(line - 3)]
    return rest + [(i + jnp.where(i >= z, 1, 0)) * 2 + 1 - x for i in range(line - 1)]


def nt_dot(a, b):
    return lax.dot_general(a, b, (((1,), (1,)), ((), ())), preferred_element_type=jnp.float32)


def gather_kernel(
    dims, own_ref, all_ref, panel_ref, part_ref, own_sem, z_send, x_send, c_send, y_send,
    recv, c_recv, y_recv, a_ref, b_ref, a_sem, b_sem,
):
    line, count, cross, rows = dims
    first = count - cross
    me, t = lax.axis_index("dp"), lax.axis_index("tensor")
    z, x, core = me // 4, me // 2 % 2, me % 2
    chips = 2 * line
    at = lambda zz, xx: zz * 2 + xx
    here = at(z, x)
    owns = (here // (chips // 2)) == t
    part = here % (chips // 2)
    per = count // (chips // 2)

    up = (jnp.minimum(z + 1, line - 1) * 4 + x * 2 + core, t)
    down = (jnp.maximum(z - 1, 0) * 4 + x * 2 + core, t)
    over = (z * 4 + (1 - x) * 2 + core, t)
    twin = (z * 4 + x * 2 + 1 - core, t)
    has_up, has_down = z < line - 1, z > 0

    barrier = pltpu.get_barrier_semaphore()
    greet = lambda dev: pl.semaphore_signal(barrier, inc=1, device_id=dev, device_id_type=MESH)
    greet(over)
    greet(twin)
    greet((me, 1 - t))
    greet(twin[:1] + (1 - t,))
    pl.when(has_up)(lambda: greet(up))
    pl.when(has_down)(lambda: greet(down))
    end = (z == 0) | (z == line - 1)
    pl.semaphore_wait(barrier, jnp.where(end, 5, 6))

    def rows_of(k):
        return pl.ds(pl.multiple_of(k * rows, rows), rows)

    def lanes_of(q):
        return pl.ds(pl.multiple_of((q * 2 + core) * LANES, LANES), LANES)

    def place(q, k):
        return all_ref.at[rows_of(k), lanes_of(q)]

    def source(q, k, own):
        return own_ref.at[rows_of(k)] if own else place(q, k)

    def along(q, k, way, own=False):
        return pltpu.make_async_remote_copy(
            src_ref=source(q, k, own), dst_ref=place(q, k), send_sem=z_send.at[way, q, k],
            recv_sem=recv.at[q, k], device_id=(down, up)[way], device_id_type=MESH)

    def across(q, k, own=False):
        return pltpu.make_async_remote_copy(
            src_ref=source(q, k, own), dst_ref=place(q, k), send_sem=x_send.at[q, k],
            recv_sem=recv.at[q, k], device_id=over, device_id_type=MESH)

    def to_twin(q, k, own=False):
        return pltpu.make_async_remote_copy(
            src_ref=source(q, k, own), dst_ref=place(q, k), send_sem=c_send.at[q, k],
            recv_sem=c_recv.at[q, k], device_id=twin, device_id_type=MESH)

    def to_panel(q, k, own=False):
        j = k % per
        half = per // 2
        return pltpu.make_async_remote_copy(
            src_ref=source(q, k, own),
            dst_ref=panel_ref.at[rows_of(j % half), lanes_of(q)],
            send_sem=y_send.at[q, j], recv_sem=y_recv.at[q * 2 + core, j % half],
            device_id=(here * 2 + j // half, 1 - t), device_id_type=MESH)

    def spread(q, k, own=False):
        to_twin(q, k, own).start()
        pl.when(owns & (k // per == part))(lambda: to_panel(q, k, own).start())

    def arrive(q, k):
        across(q, k).wait_recv()

    keep = pltpu.make_async_copy(own_ref, all_ref.at[:, lanes_of(here)], own_sem)

    @pl.loop(0, count)
    def _(k):
        pl.when(has_up)(lambda: along(here, k, 1, True).start())
        pl.when(has_down)(lambda: along(here, k, 0, True).start())
        across(here, k, True).start()
        spread(here, k, True)

    keep.start()

    def from_line(s, k, way):
        zz = z - s if way else z + s
        valid = (zz >= 0) & (zz < line)

        @pl.when(valid)
        def _():
            q = at(zz, x)
            arrive(q, k)
            pl.when(has_up if way else has_down)(lambda: along(q, k, way).start())
            pl.when(k < first)(lambda: across(q, k).start())
            spread(q, k)

    def from_cross(s, k, way):
        zz = z - s if way else z + s
        valid = (zz >= 0) & (zz < line)

        @pl.when(valid)
        def _():
            q = at(zz, 1 - x)
            arrive(q, k)
            pl.when(has_up if way else has_down)(lambda: along(q, k, way).start())
            spread(q, k)

    def relayed(s, k):
        for zz in (z - s, z + s):
            @pl.when((zz >= 0) & (zz < line))
            def _():
                q = at(zz, 1 - x)
                arrive(q, k)
                spread(q, k)

    def pair_of(q):
        return pl.ds(pl.multiple_of(q * 2 * LANES, 2 * LANES), 2 * LANES)

    def slab(j):
        return pl.ds(j * 2 * LANES, 2 * LANES)

    chosen = early(line, z, x)

    def tile_copies(k, slot):
        return [
            pltpu.make_async_copy(
                all_ref.at[rows_of(k), pair_of(q)], a_ref.at[slot, :, slab(j)], a_sem.at[slot, j]
            )
            for j, q in enumerate(chosen)
        ]

    def prepare():
        keep.wait()
        for q in chosen:
            @pl.loop(0, count)
            def _(k):
                to_twin(q, k).wait_recv()
            panel_arrived(q)
        for tile in tile_copies(0, 0):
            tile.start()
        for ours in (True, False):
            @pl.when(owns == ours)
            def _():
                width = rows * per // 2
                from_ref = (
                    all_ref.at[pl.ds(pl.multiple_of((part * 2 + core) * width, width), width)]
                    if ours else panel_ref
                )
                copies = [
                    pltpu.make_async_copy(from_ref.at[:, pair_of(q)], b_ref.at[:, slab(j)], b_sem.at[j])
                    for j, q in enumerate(chosen)
                ]
                for copy in copies:
                    copy.start()
                for copy in copies:
                    copy.wait()

    def multiply(k):
        slot = k % 2

        @pl.when(k + 1 < count)
        def _():
            for tile in tile_copies(k + 1, 1 - slot):
                tile.start()

        for tile in tile_copies(k, slot):
            tile.wait()
        part_ref[rows_of(k), :] = nt_dot(a_ref[slot], b_ref[...])

    def panel_arrived(q):
        @pl.when(jnp.logical_not(owns))
        def _():
            @pl.loop(0, per // 2)
            def _(j):
                for c in range(2):
                    piece = panel_ref.at[rows_of(j), pl.ds(pl.multiple_of((q * 2 + c) * LANES, LANES), LANES)]
                    pltpu.make_async_copy(piece, piece, y_recv.at[q * 2 + c, j]).wait()

    for s in range(1, line + 2):
        if s == 3:
            prepare()

        @pl.loop(0, count)
        def _(k):
            if s == 3:
                multiply(k)
            if s < line:
                from_line(s, k, 1)
                from_line(s, k, 0)
            if s == 1:
                q = at(z, 1 - x)
                arrive(q, k)
                spread(q, k)
            else:
                @pl.when(k < first)
                def _():
                    if s - 1 < line:
                        pl.when(end)(lambda: relayed(s - 1, k))
                    if 1 <= s - 2 < line:
                        pl.when(jnp.logical_not(end))(lambda: relayed(s - 2, k))

        if s <= line:
            @pl.loop(first, count)
            def _(k):
                if s == 1:
                    q = at(z, 1 - x)
                    pl.when(has_up)(lambda: along(q, k, 1).start())
                    pl.when(has_down)(lambda: along(q, k, 0).start())
                else:
                    from_cross(s - 1, k, 1)
                    from_cross(s - 1, k, 0)

    for q in late(line, z, x):
        @pl.loop(0, count)
        def _(k):
            to_twin(q, k).wait_recv()
        panel_arrived(q)

    @pl.loop(0, chips)
    def _(q):
        zz, mine = q // 2, q % 2 == x

        @pl.loop(0, count)
        def _(k):
            to_twin(q, k).wait_send()
            pl.when(mine & ((k < first) | (zz == z)))(lambda: across(q, k).wait_send())
            goes = mine | (k >= first)
            pl.when(goes & has_up & (zz <= z))(lambda: along(q, k, 1).wait_send())
            pl.when(goes & has_down & (zz >= z))(lambda: along(q, k, 0).wait_send())
            pl.when(owns & (k // per == part))(lambda: to_panel(q, k).wait_send())


def gather(own, dims, width, tokens):
    line, count, cross, rows = dims
    chips = 2 * line
    per = count // line
    sem = pltpu.SemaphoreType.DMA
    hidden = own.shape[0]
    return pl.pallas_call(
        functools.partial(gather_kernel, dims),
        out_shape=(
            jax.ShapeDtypeStruct((hidden, tokens), jnp.bfloat16),
            jax.ShapeDtypeStruct((width, tokens), jnp.bfloat16),
            pltpu.VMEM((hidden, width), jnp.float32),
        ),
        in_specs=[pl.BlockSpec(memory_space=pl.ANY)],
        out_specs=(
            pl.BlockSpec(memory_space=pl.ANY),
            pl.BlockSpec(memory_space=pl.ANY),
            pl.BlockSpec(memory_space=pltpu.VMEM),
        ),
        scratch_shapes=[
            sem(()),
            sem((2, chips, count)),
            sem((chips, count)),
            sem((chips, count)),
            sem((chips, per)),
            sem((chips, count)),
            sem((chips, count)),
            sem((2 * chips, per // 2)),
            pltpu.VMEM((2, rows, 8 * LANES), jnp.bfloat16),
            pltpu.VMEM((width, 8 * LANES), jnp.bfloat16),
            sem((2, 4)),
            sem((4,)),
        ],
        compiler_params=pltpu.CompilerParams(
            collective_id=0, has_side_effects=True, vmem_limit_bytes=36 * 2**20
        ),
    )(own)


def matmul_kernel(total, width, left, chips_ref, *refs):
    pieces, (all_ref, panel_ref, part_ref, o_ref, b_ref, sem) = refs[:left], refs[left:]
    me, t = lax.axis_index("dp"), lax.axis_index("tensor")
    ratio = lax.axis_size("dp") // lax.axis_size("tensor")
    step, tile = pl.program_id(0), o_ref.shape[0]

    @pl.when(step == 0)
    def _():
        for ours in (True, False):
            @pl.when((me // ratio == t) == ours)
            def _():
                rows = pl.ds(pl.multiple_of(me % ratio * width, LANES), width)
                from_ref = all_ref.at[rows] if ours else panel_ref
                copies = [
                    pltpu.make_async_copy(
                        from_ref.at[:, pl.ds(pl.multiple_of(chips_ref[j] * 2 * LANES, LANES), 2 * LANES)],
                        b_ref.at[:, pl.ds(j * 2 * LANES, 2 * LANES)],
                        sem.at[j],
                    )
                    for j in range(left)
                ]
                for copy in copies:
                    copy.start()
                for copy in copies:
                    copy.wait()

    a = jnp.concatenate([piece[...] for piece in pieces], axis=1)
    done = part_ref[pl.ds(pl.multiple_of(step * tile, tile), tile), :]
    o_ref[...] = (done + nt_dot(a, b_ref[...])) * (1.0 / total)


def matmul(everything, panel, part, chips, tile):
    hidden, tokens = everything.shape
    width = panel.shape[0]
    left = chips.shape[0]
    everything = pltpu.with_memory_space_constraint(everything, pltpu.HBM)
    panel = pltpu.with_memory_space_constraint(panel, pltpu.HBM)
    part = pltpu.with_memory_space_constraint(part, pltpu.VMEM)

    def piece(j):
        return pl.BlockSpec((tile, 2 * LANES), lambda i, chips_ref: (i, chips_ref[j]))

    return pl.pallas_call(
        functools.partial(matmul_kernel, tokens, width, left),
        grid_spec=pltpu.PrefetchScalarGridSpec(
            num_scalar_prefetch=1,
            grid=(hidden // tile,),
            in_specs=[piece(j) for j in range(left)] + [
                pl.BlockSpec(memory_space=pltpu.HBM),
                pl.BlockSpec(memory_space=pltpu.HBM),
                pl.BlockSpec(memory_space=pltpu.VMEM),
            ],
            out_specs=pl.BlockSpec((tile, width), lambda i, chips_ref: (i, 0)),
            scratch_shapes=[
                pltpu.VMEM((width, left * 2 * LANES), jnp.bfloat16),
                pltpu.SemaphoreType.DMA((left,)),
            ],
        ),
        out_shape=jax.ShapeDtypeStruct((hidden, width), jnp.float32),
        compiler_params=pltpu.CompilerParams(vmem_limit_bytes=36 * 2**20),
    )(chips, *[everything] * (left + 1), panel, part)


def shards(grad_hidden, gate):
    tensor_count, data_count = lax.axis_size("tensor"), lax.axis_size("dp")
    mine, hidden = grad_hidden.shape
    width = hidden * tensor_count // data_count
    tokens = mine * data_count
    count = data_count
    fits = (
        tensor_count == 2 and data_count % 4 == 0 and data_count >= 16 and mine == LANES and width % LANES == 0
        and hidden % (16 * count) == 0 and tokens & (tokens - 1) == 0 and hidden % 1024 == 0
    )
    if not fits:
        return plain(grad_hidden, gate)
    line = data_count // 4
    cross = round(count / (2 * (line - 1)))
    dims = (line, count, cross, hidden // count)
    own = flip(grad_hidden, gate, 1024)
    everything, panel, part = gather(own, dims, width, tokens)
    index = lax.axis_index("dp")
    chips = jnp.stack(late(line, index // 4, index // 2 % 2)).astype(jnp.int32)
    return matmul(everything, panel, part, chips, 512)


def solution(mesh):
    return jax.shard_map(
        shards,
        mesh=mesh,
        in_specs=(P("dp", "tensor"), P("dp", "tensor")),
        out_specs=P("tensor", "dp"),
        check_vma=False,
    )
```

```python
import functools

import jax
import jax.numpy as jnp
from jax import lax
from jax.experimental import pallas as pl
from jax.experimental.pallas import tpu as pltpu
from jax.sharding import PartitionSpec as P

MESH = pl.DeviceIdType.MESH
LANES = 128


def activations(grad_hidden, gate):
    return (grad_hidden.astype(jnp.float32) * jax.nn.silu(gate.astype(jnp.float32))).astype(
        jnp.bfloat16
    )


def plain(grad_hidden, gate):
    up_grad = activations(grad_hidden, gate)
    tensor_count = lax.axis_size("tensor")
    data_count = lax.axis_size("dp")
    col_width = up_grad.shape[1] * tensor_count // data_count
    ratio = data_count // tensor_count
    data_index = lax.axis_index("dp")
    owner = data_index // ratio
    offset = data_index % ratio * col_width
    contract = (((0,), (0,)), ((), ()))
    total_tokens = up_grad.shape[0] * data_count
    rows_all = lax.all_gather(up_grad, "dp", axis=0, tiled=True)
    panel = lax.dynamic_slice_in_dim(rows_all, offset, col_width, 1)
    slices = lax.all_gather(panel, "tensor", axis=1, tiled=True)
    cols_all = lax.dynamic_slice_in_dim(slices, owner * col_width, col_width, 1)
    summed = lax.dot_general(rows_all, cols_all, contract, preferred_element_type=jnp.float32)
    return summed / total_tokens


def flip_kernel(g_ref, v_ref, o_ref):
    v = v_ref[...].astype(jnp.float32)
    u = g_ref[...].astype(jnp.float32) * (v / (1.0 + jnp.exp(-v)))
    o_ref[...] = u.astype(jnp.bfloat16).T


def flip(grad_hidden, gate, width):
    tokens, hidden = grad_hidden.shape
    return pl.pallas_call(
        flip_kernel,
        grid=(hidden // width,),
        in_specs=[pl.BlockSpec((tokens, width), lambda i: (0, i))] * 2,
        out_specs=pl.BlockSpec((width, tokens), lambda i: (i, 0)),
        out_shape=jax.ShapeDtypeStruct((hidden, tokens), jnp.bfloat16),
    )(grad_hidden, gate)


def early(line, z, x):
    end, low, high = (z == 0) | (z == line - 1), z == 0, z == line - 1
    near = jnp.where(low, 1, z - 1)
    after = jnp.where(low, 2, jnp.where(high, line - 3, z + 1))
    inner = jnp.where(z < line - 2, z + 2, z - 2) * 2 + x
    far = jnp.where(low, 3, line - 4) * 2 + x
    other = near * 2 + 1 - x
    five = [z * 2 + x, z * 2 + 1 - x, near * 2 + x, after * 2 + x, jnp.where(end, other, inner)]
    return five + [jnp.where(end, far, other)]


def member(q, chosen):
    return functools.reduce(jnp.logical_or, [q == c for c in chosen])


def late(line, z, x):
    chosen = early(line, z, x)
    left = 2 * line - len(chosen)
    picked, rank = [jnp.int32(0)] * left, jnp.int32(0)
    for q in range(2 * line):
        free = jnp.logical_not(member(q, chosen))
        picked = [jnp.where(free & (rank == j), q, p) for j, p in enumerate(picked)]
        rank = rank + free.astype(jnp.int32)
    return picked


def nt_dot(a, b):
    return lax.dot_general(a, b, (((1,), (1,)), ((), ())), preferred_element_type=jnp.float32)


def gather_kernel(
    dims, own_ref, all_ref, panel_ref, part_ref, own_sem, z_send, x_send, c_send, y_send,
    recv, c_recv, y_recv, a_ref, b_ref, a_sem, b_sem,
):
    line, count, cross, rows = dims
    first = count - cross
    me, t = lax.axis_index("dp"), lax.axis_index("tensor")
    z, x, core = me // 4, me // 2 % 2, me % 2
    chips = 2 * line
    at = lambda zz, xx: zz * 2 + xx
    here = at(z, x)
    owns = (here // (chips // 2)) == t
    part = here % (chips // 2)
    per = count // (chips // 2)

    up = (jnp.minimum(z + 1, line - 1) * 4 + x * 2 + core, t)
    down = (jnp.maximum(z - 1, 0) * 4 + x * 2 + core, t)
    over = (z * 4 + (1 - x) * 2 + core, t)
    twin = (z * 4 + x * 2 + 1 - core, t)
    has_up, has_down = z < line - 1, z > 0

    barrier = pltpu.get_barrier_semaphore()
    greet = lambda dev: pl.semaphore_signal(barrier, inc=1, device_id=dev, device_id_type=MESH)
    greet(over)
    greet(twin)
    greet((me, 1 - t))
    greet(twin[:1] + (1 - t,))
    pl.when(has_up)(lambda: greet(up))
    pl.when(has_down)(lambda: greet(down))
    end = (z == 0) | (z == line - 1)
    pl.semaphore_wait(barrier, jnp.where(end, 5, 6))

    def rows_of(k):
        return pl.ds(pl.multiple_of(k * rows, rows), rows)

    def lanes_of(q):
        return pl.ds(pl.multiple_of((q * 2 + core) * LANES, LANES), LANES)

    def place(q, k):
        return all_ref.at[rows_of(k), lanes_of(q)]

    def source(q, k, own):
        return own_ref.at[rows_of(k)] if own else place(q, k)

    def along(q, k, way, own=False):
        return pltpu.make_async_remote_copy(
            src_ref=source(q, k, own), dst_ref=place(q, k), send_sem=z_send.at[way, q, k],
            recv_sem=recv.at[q, k], device_id=(down, up)[way], device_id_type=MESH)

    def across(q, k, own=False):
        return pltpu.make_async_remote_copy(
            src_ref=source(q, k, own), dst_ref=place(q, k), send_sem=x_send.at[q, k],
            recv_sem=recv.at[q, k], device_id=over, device_id_type=MESH)

    def to_twin(q, k, own=False):
        return pltpu.make_async_remote_copy(
            src_ref=source(q, k, own), dst_ref=place(q, k), send_sem=c_send.at[q, k],
            recv_sem=c_recv.at[q, k], device_id=twin, device_id_type=MESH)

    def to_panel(q, k, own=False):
        j = k % per
        half = per // 2
        return pltpu.make_async_remote_copy(
            src_ref=source(q, k, own),
            dst_ref=panel_ref.at[rows_of(j % half), lanes_of(q)],
            send_sem=y_send.at[q, j], recv_sem=y_recv.at[q * 2 + core, j % half],
            device_id=(here * 2 + j // half, 1 - t), device_id_type=MESH)

    def spread(q, k, own=False):
        to_twin(q, k, own).start()
        pl.when(owns & (k // per == part))(lambda: to_panel(q, k, own).start())

    def arrive(q, k):
        across(q, k).wait_recv()

    keep = pltpu.make_async_copy(own_ref, all_ref.at[:, lanes_of(here)], own_sem)

    @pl.loop(0, count)
    def _(k):
        pl.when(has_up)(lambda: along(here, k, 1, True).start())
        pl.when(has_down)(lambda: along(here, k, 0, True).start())
        across(here, k, True).start()
        spread(here, k, True)

    keep.start()

    def from_line(s, k, way):
        zz = z - s if way else z + s
        valid = (zz >= 0) & (zz < line)

        @pl.when(valid)
        def _():
            q = at(zz, x)
            arrive(q, k)
            pl.when(has_up if way else has_down)(lambda: along(q, k, way).start())
            pl.when(k < first)(lambda: across(q, k).start())
            spread(q, k)

    def from_cross(s, k, way):
        zz = z - s if way else z + s
        valid = (zz >= 0) & (zz < line)

        @pl.when(valid)
        def _():
            q = at(zz, 1 - x)
            arrive(q, k)
            pl.when(has_up if way else has_down)(lambda: along(q, k, way).start())
            spread(q, k)

    def relayed(s, k):
        for zz in (z - s, z + s):
            @pl.when((zz >= 0) & (zz < line))
            def _():
                q = at(zz, 1 - x)
                arrive(q, k)
                spread(q, k)

    def pair_of(q):
        return pl.ds(pl.multiple_of(q * 2 * LANES, 2 * LANES), 2 * LANES)

    def slab(j):
        return pl.ds(j * 2 * LANES, 2 * LANES)

    chosen = early(line, z, x)
    first_group, second_group = chosen[:-1], chosen[-1:]

    def tile_copies(group, k, slot):
        return [
            pltpu.make_async_copy(
                all_ref.at[rows_of(k), pair_of(q)], a_ref.at[slot, :, slab(j)], a_sem.at[slot, j]
            )
            for j, q in enumerate(group)
        ]

    def prepare(group):
        for q in group:
            @pl.loop(0, count)
            def _(k):
                to_twin(q, k).wait_recv()
            panel_arrived(q)
        for tile in tile_copies(group, 0, 0):
            tile.start()
        for ours in (True, False):
            @pl.when(owns == ours)
            def _():
                width = rows * per // 2
                from_ref = (
                    all_ref.at[pl.ds(pl.multiple_of((part * 2 + core) * width, width), width)]
                    if ours else panel_ref
                )
                copies = [
                    pltpu.make_async_copy(from_ref.at[:, pair_of(q)], b_ref.at[:, slab(j)], b_sem.at[j])
                    for j, q in enumerate(group)
                ]
                for copy in copies:
                    copy.start()
                for copy in copies:
                    copy.wait()

    def multiply(group, k, add):
        slot = k % 2

        @pl.when(k + 1 < count)
        def _():
            for tile in tile_copies(group, k + 1, 1 - slot):
                tile.start()

        for tile in tile_copies(group, k, slot):
            tile.wait()
        span = pl.ds(0, len(group) * 2 * LANES)
        product = nt_dot(a_ref[slot, :, span], b_ref[:, span])
        if add:
            product += part_ref[rows_of(k), :]
        part_ref[rows_of(k), :] = product

    def panel_arrived(q):
        @pl.when(jnp.logical_not(owns))
        def _():
            @pl.loop(0, per // 2)
            def _(j):
                for c in range(2):
                    piece = panel_ref.at[rows_of(j), pl.ds(pl.multiple_of((q * 2 + c) * LANES, LANES), LANES)]
                    pltpu.make_async_copy(piece, piece, y_recv.at[q * 2 + c, j]).wait()

    for s in range(1, line + 2):
        if s == 3:
            keep.wait()
            prepare(first_group)
        if s == 4:
            prepare(second_group)

        @pl.loop(0, count)
        def _(k):
            if s == 3:
                multiply(first_group, k, False)
            if s == 4:
                multiply(second_group, k, True)
            if s < line:
                from_line(s, k, 1)
                from_line(s, k, 0)
            if s == 1:
                q = at(z, 1 - x)
                arrive(q, k)
                spread(q, k)
            else:
                @pl.when(k < first)
                def _():
                    if s - 1 < line:
                        pl.when(end)(lambda: relayed(s - 1, k))
                    if 1 <= s - 2 < line:
                        pl.when(jnp.logical_not(end))(lambda: relayed(s - 2, k))

        if s <= line:
            @pl.loop(first, count)
            def _(k):
                if s == 1:
                    q = at(z, 1 - x)
                    pl.when(has_up)(lambda: along(q, k, 1).start())
                    pl.when(has_down)(lambda: along(q, k, 0).start())
                else:
                    from_cross(s - 1, k, 1)
                    from_cross(s - 1, k, 0)

    @pl.loop(0, chips)
    def _(q):
        @pl.when(jnp.logical_not(member(q, chosen)))
        def _():
            @pl.loop(0, count)
            def _(k):
                to_twin(q, k).wait_recv()
            panel_arrived(q)

    @pl.loop(0, chips)
    def _(q):
        zz, mine = q // 2, q % 2 == x

        @pl.loop(0, count)
        def _(k):
            to_twin(q, k).wait_send()
            pl.when(mine & ((k < first) | (zz == z)))(lambda: across(q, k).wait_send())
            goes = mine | (k >= first)
            pl.when(goes & has_up & (zz <= z))(lambda: along(q, k, 1).wait_send())
            pl.when(goes & has_down & (zz >= z))(lambda: along(q, k, 0).wait_send())
            pl.when(owns & (k // per == part))(lambda: to_panel(q, k).wait_send())


def gather(own, dims, width, tokens):
    line, count, cross, rows = dims
    chips = 2 * line
    per = count // line
    sem = pltpu.SemaphoreType.DMA
    hidden = own.shape[0]
    return pl.pallas_call(
        functools.partial(gather_kernel, dims),
        out_shape=(
            jax.ShapeDtypeStruct((hidden, tokens), jnp.bfloat16),
            jax.ShapeDtypeStruct((width, tokens), jnp.bfloat16),
            pltpu.VMEM((hidden, width), jnp.float32),
        ),
        in_specs=[pl.BlockSpec(memory_space=pl.ANY)],
        out_specs=(
            pl.BlockSpec(memory_space=pl.ANY),
            pl.BlockSpec(memory_space=pl.ANY),
            pl.BlockSpec(memory_space=pltpu.VMEM),
        ),
        scratch_shapes=[
            sem(()),
            sem((2, chips, count)),
            sem((chips, count)),
            sem((chips, count)),
            sem((chips, per)),
            sem((chips, count)),
            sem((chips, count)),
            sem((2 * chips, per // 2)),
            pltpu.VMEM((2, rows, 10 * LANES), jnp.bfloat16),
            pltpu.VMEM((width, 10 * LANES), jnp.bfloat16),
            sem((2, 5)),
            sem((5,)),
        ],
        compiler_params=pltpu.CompilerParams(
            collective_id=0, has_side_effects=True, vmem_limit_bytes=36 * 2**20
        ),
    )(own)


def matmul_kernel(total, width, left, chips_ref, *refs):
    pieces, (all_ref, panel_ref, part_ref, o_ref, b_ref, sem) = refs[:left], refs[left:]
    me, t = lax.axis_index("dp"), lax.axis_index("tensor")
    ratio = lax.axis_size("dp") // lax.axis_size("tensor")
    step, tile = pl.program_id(0), o_ref.shape[0]

    @pl.when(step == 0)
    def _():
        for ours in (True, False):
            @pl.when((me // ratio == t) == ours)
            def _():
                rows = pl.ds(pl.multiple_of(me % ratio * width, LANES), width)
                from_ref = all_ref.at[rows] if ours else panel_ref
                copies = [
                    pltpu.make_async_copy(
                        from_ref.at[:, pl.ds(pl.multiple_of(chips_ref[j] * 2 * LANES, LANES), 2 * LANES)],
                        b_ref.at[:, pl.ds(j * 2 * LANES, 2 * LANES)],
                        sem.at[j],
                    )
                    for j in range(left)
                ]
                for copy in copies:
                    copy.start()
                for copy in copies:
                    copy.wait()

    a = jnp.concatenate([piece[...] for piece in pieces], axis=1)
    done = part_ref[pl.ds(pl.multiple_of(step * tile, tile), tile), :]
    o_ref[...] = (done + nt_dot(a, b_ref[...])) * (1.0 / total)


def matmul(everything, panel, part, chips, tile):
    hidden, tokens = everything.shape
    width = panel.shape[0]
    left = chips.shape[0]
    everything = pltpu.with_memory_space_constraint(everything, pltpu.HBM)
    panel = pltpu.with_memory_space_constraint(panel, pltpu.HBM)
    part = pltpu.with_memory_space_constraint(part, pltpu.VMEM)

    def piece(j):
        return pl.BlockSpec((tile, 2 * LANES), lambda i, chips_ref: (i, chips_ref[j]))

    return pl.pallas_call(
        functools.partial(matmul_kernel, tokens, width, left),
        grid_spec=pltpu.PrefetchScalarGridSpec(
            num_scalar_prefetch=1,
            grid=(hidden // tile,),
            in_specs=[piece(j) for j in range(left)] + [
                pl.BlockSpec(memory_space=pltpu.HBM),
                pl.BlockSpec(memory_space=pltpu.HBM),
                pl.BlockSpec(memory_space=pltpu.VMEM),
            ],
            out_specs=pl.BlockSpec((tile, width), lambda i, chips_ref: (i, 0)),
            scratch_shapes=[
                pltpu.VMEM((width, left * 2 * LANES), jnp.bfloat16),
                pltpu.SemaphoreType.DMA((left,)),
            ],
        ),
        out_shape=jax.ShapeDtypeStruct((hidden, width), jnp.float32),
        compiler_params=pltpu.CompilerParams(vmem_limit_bytes=36 * 2**20),
    )(chips, *[everything] * (left + 1), panel, part)


def shards(grad_hidden, gate):
    tensor_count, data_count = lax.axis_size("tensor"), lax.axis_size("dp")
    mine, hidden = grad_hidden.shape
    width = hidden * tensor_count // data_count
    tokens = mine * data_count
    count = data_count
    fits = (
        tensor_count == 2 and data_count % 4 == 0 and data_count >= 16 and mine == LANES and width % LANES == 0
        and hidden % (16 * count) == 0 and tokens & (tokens - 1) == 0 and hidden % 1024 == 0
    )
    if not fits:
        return plain(grad_hidden, gate)
    line = data_count // 4
    cross = round(count / (2 * (line - 1)))
    dims = (line, count, cross, hidden // count)
    own = flip(grad_hidden, gate, 1024)
    everything, panel, part = gather(own, dims, width, tokens)
    index = lax.axis_index("dp")
    chips = jnp.stack(late(line, index // 4, index // 2 % 2)).astype(jnp.int32)
    return matmul(everything, panel, part, chips, 512)


def solution(mesh):
    return jax.shard_map(
        shards,
        mesh=mesh,
        in_specs=(P("dp", "tensor"), P("dp", "tensor")),
        out_specs=P("tensor", "dp"),
        check_vma=False,
    )
```
